256 devices in a mesh: rows: 64 (over z, y, core), grp: 4 (over x).
Axes of the slice: x: 4, y: 4, z: 8, core: 2. Of those that a mesh axis runs over, the one named last changes fastest.
Arguments:
- cholesky_vectors: bfloat16 [524288, 2048], P(('rows', 'grp'))
- integral_columns: float32 [524288, 64], P(('rows', 'grp'))
- residual_diag: float32 [524288], P(('rows', 'grp')), may hold values from 40 to 120
- slot_pair_block: int32 [4096], P(('rows', 'grp')), may hold values from 0 to 4095, as said below
- block_live: int32 [4096], P(('rows', 'grp')), may hold values from 0 to 1, as said below
- pivots: int32 [64], replicated, may hold values from 0 to 524287, as said below
Outputs:
- new_columns: float32 [524288, 64], P(('rows', 'grp'))
- relative_diag: float32 [524288], P(('rows', 'grp'))
- peak: float32 [], replicated
The draws below stay inside these ranges and needn't reach their ends.
Inputs may be any that keep to these rules, and one draw needn't show every extreme that they name: `slot_pair_block`: each block number appears once. `block_live`: slots s * 16 to s * 16 + 15 are those of device s; each device has 1 to 12 surviving slots, and some device has exactly 12. Distinct; every pivot lies in a surviving slot; each device's slots hold at most 1 pivots, and some device holds exactly 1.
All inputs are finite; a program needn't handle non-finite values.
Results may differ from the reference program's by a relative error of at most 0.0003.
Values sent between devices are 32-bit elements; how exact they have to be, the bound alone decides.
No kernel may reach another device: no remote copies, remote signals or barrier semaphores. Data moves between devices by JAX's collectives and lax.ppermute only.
A program may use at most 64 MiB of HBM per device.

```python
import jax
import jax.numpy as jnp
from jax import lax

BLK = 128
PIV = 64
K = 2048
SLOTS = 16
LIVE_MOST = 12
HOLDERS = 256
TOTAL_SLOTS = 4096
NROWS = 524288
PIV_MOST = 1


def slot_layout(key):
    base = jax.random.fold_in(key, 7)
    random_keys = jax.random.split(base, 8)
    slot_pair_block = jax.random.permutation(random_keys[0], TOTAL_SLOTS).astype(jnp.int32)
    small_count = jax.random.randint(random_keys[1], (HOLDERS,), 1, max(2, LIVE_MOST // 3 + 1))
    heavy = jax.random.randint(random_keys[2], (HOLDERS,), 0, 4) == 0
    counts = jnp.where(heavy, LIVE_MOST, small_count)
    forced = jax.random.randint(random_keys[3], (), 0, HOLDERS)
    counts = jnp.where(jnp.arange(HOLDERS) == forced, LIVE_MOST, counts)
    scores = jax.random.randint(random_keys[4], (HOLDERS, SLOTS), 0, 1000) * SLOTS + jnp.arange(SLOTS)[None, :]
    ranks = jnp.argsort(jnp.argsort(scores, axis=1), axis=1)
    live = (ranks < counts[:, None]).astype(jnp.int32)
    holder_order = jax.random.permutation(random_keys[5], HOLDERS)
    index = jnp.arange(PIV)
    holder = holder_order[index % HOLDERS]
    within = index // HOLDERS
    choose = live[holder] * (SLOTS * 1000) + jax.random.randint(random_keys[6], (PIV, SLOTS), 0, 1000) * SLOTS + jnp.arange(SLOTS)[None, :]
    slot = jnp.argmax(choose, axis=1)
    offset = jax.random.randint(random_keys[7], (PIV,), 0, BLK // PIV_MOST) * PIV_MOST + within
    global_slot = holder * SLOTS + slot
    pivot_ids = (slot_pair_block[global_slot] * BLK + offset).astype(jnp.int32)
    pivot_rows = (global_slot * BLK + offset).astype(jnp.int32)
    return (slot_pair_block, live.reshape(-1), pivot_ids, pivot_rows)


def draw_slot_pair_block(key, part):
    return slot_layout(key)[0]


def draw_block_live(key, part):
    return slot_layout(key)[1]


def draw_pivots(key, part):
    return slot_layout(key)[2]


def draw_cholesky_vectors(key, part):
    inner = jax.random.fold_in(key, 31)
    spread = K ** (-0.25)
    values = jax.random.normal(inner, (NROWS, K), jnp.float32)
    return (values * spread).astype(jnp.bfloat16)


def draw_integral_columns(key, part):
    vectors = draw_cholesky_vectors(key, part)
    pivot_rows = slot_layout(key)[3]
    picked = vectors[pivot_rows]
    gram = jnp.dot(picked, picked.T, preferred_element_type=jnp.float32)
    random_keys = jax.random.split(jax.random.fold_in(key, 53), 3)
    diag_part = jax.random.uniform(random_keys[0], (PIV,), jnp.float32, 14.0, 40.0)
    coupling = jax.random.uniform(random_keys[1], (PIV, PIV), jnp.float32, -0.4, 0.4)
    coupling = (coupling + coupling.T) * 0.5 * (1.0 - jnp.eye(PIV, dtype=jnp.float32))
    block = gram + jnp.diag(diag_part) + coupling
    filler = jax.random.normal(random_keys[2], (NROWS, PIV), jnp.float32)
    return filler.at[pivot_rows].set(block)


def levels(stream_key, dims, cuts, least, top_value):
    factor_of, own = 1.0, jax.random.fold_in(stream_key, 6)
    for axis_at, shards_of in cuts:
        steps = jnp.exp(jax.random.uniform(jax.random.fold_in(own, axis_at), (shards_of,), jnp.float32, least / len(cuts), top_value / len(cuts)))
        factor_of = factor_of * jnp.repeat(steps, dims[axis_at] // shards_of).reshape([-1 if axis == axis_at else 1 for axis in range(len(dims))])
    return factor_of


def setup_inputs(seed: int = 0) -> dict:
    seeds = jax.random.split(jax.random.key(seed), 7)
    cholesky_vectors = draw_cholesky_vectors(jax.random.fold_in(seeds[6], 71), 0)
    integral_columns = draw_integral_columns(jax.random.fold_in(seeds[6], 71), 0)
    residual_diag = jnp.clip(40.0 + 80.0 * jax.random.uniform(seeds[2], (NROWS,), jnp.float32) ** levels(seeds[2], (NROWS,), ((0, 256),), -0.2, 0.2), 40.0, 120.0)
    slot_pair_block = draw_slot_pair_block(jax.random.fold_in(seeds[6], 71), 0)
    block_live = draw_block_live(jax.random.fold_in(seeds[6], 71), 0)
    pivots = draw_pivots(jax.random.fold_in(seeds[6], 71), 0)
    return dict(cholesky_vectors=cholesky_vectors, integral_columns=integral_columns, residual_diag=residual_diag, slot_pair_block=slot_pair_block, block_live=block_live, pivots=pivots)


def reference(cholesky_vectors, integral_columns, residual_diag, slot_pair_block, block_live, pivots):
    block_slot_lookup = jnp.zeros((TOTAL_SLOTS,), jnp.int32).at[slot_pair_block].set(jnp.arange(TOTAL_SLOTS, dtype=jnp.int32))
    pivot_rows = (block_slot_lookup[pivots // BLK] * BLK + pivots % BLK).astype(jnp.int32)
    picked = cholesky_vectors[pivot_rows]
    pivot_block = integral_columns[pivot_rows]
    gram = jnp.dot(picked.astype(jnp.float32), picked.T.astype(jnp.float32), preferred_element_type=jnp.float32)
    lower_factor = jnp.linalg.cholesky(pivot_block - gram)
    remain = integral_columns - jnp.dot(cholesky_vectors.astype(jnp.float32), picked.T.astype(jnp.float32), preferred_element_type=jnp.float32)
    columns = lax.linalg.triangular_solve(lower_factor, remain, left_side=False, lower=True, transpose_a=True)
    live_rows = jnp.repeat(block_live, BLK) > 0
    columns = jnp.where(live_rows[:, None], columns, 0.0)
    updated = jnp.where(live_rows, residual_diag - jnp.sum(columns * columns, axis=1), residual_diag)
    is_pivot = jnp.zeros((NROWS,), jnp.int32).at[pivot_rows].set(1) > 0
    updated = jnp.where(is_pivot, 0.0, updated)
    peak = jnp.max(jnp.where(live_rows, updated, 0.0))
    return (columns, updated / peak, peak)
```

```python
import jax
import jax.numpy as jnp
from jax import lax
from jax.experimental import pallas as pl
from jax.experimental.pallas import tpu as pltpu
from jax.sharding import Mesh
from jax.sharding import PartitionSpec as P

AXES = ("z", "y", "c", "x")
LANES = 128
LIVE_MOST = 12
VMEM = pl.BlockSpec(memory_space=pltpu.VMEM)
SMEM = pl.BlockSpec(memory_space=pltpu.SMEM)
ANY = pl.BlockSpec(memory_space=pltpu.HBM)
F32 = jnp.float32
BF16 = jnp.bfloat16


def iota(shape, dim):
    return lax.broadcasted_iota(jnp.int32, shape, dim)


def dot_lanes(a, b, **kw):
    return lax.dot_general(a, b, (((1,), (1,)), ((), ())), preferred_element_type=F32, **kw)


def dot(a, b):
    return lax.dot_general(a, b, (((1,), (0,)), ((), ())), preferred_element_type=F32)


def halves(a):
    hi = a.astype(BF16)
    return hi, (a - hi.astype(F32)).astype(BF16)


def pick_kernel(count, piv_ref, spb_ref, vec_ref, ict_ref, out_ref, meta_ref, vbuf, ibuf, sems):
    piv = piv_ref[...]
    group, offset = piv >> 7, piv & (LANES - 1)
    code = jnp.zeros(piv.shape, jnp.int32)
    for s in range(spb_ref.shape[0]):
        code = jnp.where(
            group == spb_ref[s], (s * LANES + offset) * count + iota(piv.shape, 1) + 1, code
        )
    best = jnp.max(code.astype(F32)).astype(jnp.int32)
    has = best > 0
    at = jnp.maximum(best - 1, 0)
    row, q = at // count, at % count
    vcopy = pltpu.make_async_copy(
        vec_ref.at[pl.ds(pl.multiple_of((row // 8) * 8, 8), 8), :], vbuf, sems.at[0]
    )
    icopy = pltpu.make_async_copy(
        ict_ref.at[:, pl.ds(pl.multiple_of((row // LANES) * LANES, LANES), LANES)],
        ibuf.at[pl.ds(count, count), :],
        sems.at[1],
    )
    vcopy.start()
    icopy.start()
    meta_ref[0] = jnp.where(has, row, -1)
    ibuf[pl.ds(0, count), :] = jnp.zeros((count, LANES), F32)
    k = vbuf.shape[1]
    vcopy.wait()
    mine = (iota(vbuf.shape, 0) == row % 8) & has
    vrow = jnp.sum(jnp.where(mine, vbuf[...].astype(F32), 0.0), axis=0, keepdims=True)
    out_ref[:, pl.ds(0, k)] = jnp.broadcast_to(vrow, (out_ref.shape[0], k))
    icopy.wait()
    tile = (out_ref.shape[0], LANES)
    hot = jnp.where((iota(tile, 1) == row % LANES) & has, 1.0, 0.0)
    ints = dot_lanes(hot, ibuf[...], precision=lax.Precision.HIGHEST)
    index = jnp.where(has, q + 1, 0).astype(F32)
    out_ref[:, pl.ds(k, LANES)] = jnp.where(iota(tile, 1) == 0, index, ints)


def pick(pivots, spb, vec, ict, copies):
    count, k = pivots.shape[1], vec.shape[1]
    return pl.pallas_call(
        lambda *refs: pick_kernel(count, *refs),
        out_shape=(
            jax.ShapeDtypeStruct((copies, k + LANES), F32),
            jax.ShapeDtypeStruct((1,), jnp.int32),
        ),
        in_specs=[VMEM, SMEM, ANY, ANY],
        out_specs=(VMEM, SMEM),
        scratch_shapes=[
            pltpu.VMEM((8, k), BF16),
            pltpu.VMEM((2 * count, LANES), F32),
            pltpu.SemaphoreType.DMA((2,)),
        ],
        compiler_params=pltpu.CompilerParams(vmem_limit_bytes=63 << 20),
        name="pick",
    )(pivots, spb, vec, ict)


def place_kernel(rows_ref, out_ref):
    k = rows_ref.shape[1] - LANES
    tail = rows_ref[:, pl.ds(k, LANES)]
    hot = tail[:, 0:1].astype(jnp.int32) - 1 == iota((rows_ref.shape[0], out_ref.shape[0]), 1)
    hot = jnp.where(hot, 1.0, 0.0).astype(BF16)
    turn = (((0,), (0,)), ((), ()))
    out_ref[:, pl.ds(0, k)] = lax.dot_general(
        hot, rows_ref[:, pl.ds(0, k)].astype(BF16), turn, preferred_element_type=F32
    )
    total = jnp.zeros((out_ref.shape[0], LANES), F32)
    for _ in range(3):
        part = tail.astype(BF16)
        tail = tail - part.astype(F32)
        total += lax.dot_general(hot, part, turn, preferred_element_type=F32)
    out_ref[:, pl.ds(k, LANES)] = total


def place(rows, count):
    return pl.pallas_call(
        place_kernel,
        out_shape=jax.ShapeDtypeStruct((count, rows.shape[1]), F32),
        in_specs=[VMEM],
        out_specs=VMEM,
        compiler_params=pltpu.CompilerParams(vmem_limit_bytes=8 << 20),
        name="place",
    )(rows)


def inverse_factor(m_ref, d_ref, count):
    for at in range(count):
        m = m_ref[...]
        row = m_ref[pl.ds(at, 1), :]
        d = row[:, count + at : count + at + 1]
        col = m[:, count + at : count + at + 1] / d
        below = iota((count, 1), 0) > at
        m_ref[...] = m - jnp.where(below, col, 0.0) * row
        d_ref[pl.ds(at, 1), :] = jnp.broadcast_to(d, (1, LANES))
    return m_ref[:, pl.ds(0, count)] * lax.rsqrt(d_ref[:, pl.ds(0, count)])


def step_kernel(
    here_ref, there_ref, vec_ref, ict_ref, diag_ref, live_ref, meta_ref,
    cols_ref, upd_ref, top_ref,
    vbuf, ibuf, dbuf, padded, m_ref, d_ref, remain, slots, vsems, sems,
):
    most, blk, k = vbuf.shape
    count = here_ref.shape[0]
    total = live_ref.shape[0]
    found = jnp.int32(0)
    for s in range(total):
        slots[found] = s
        found += live_ref[s]
    for s in range(total):
        slots[found] = s
        found += 1 - live_ref[s]
    vcopies = []
    for j in range(most):
        start = pl.multiple_of(slots[j] * blk, blk)
        vcopies.append(
            pltpu.make_async_copy(vec_ref.at[pl.ds(start, blk), :], vbuf.at[j], vsems.at[j])
        )
        vcopies[-1].start()
    icopy = pltpu.make_async_copy(ict_ref, ibuf, sems.at[0])
    icopy.start()
    dcopy = pltpu.make_async_copy(diag_ref, dbuf, sems.at[1])
    dcopy.start()

    cols_ref[...] = jnp.zeros(cols_ref.shape, F32)
    picked = (here_ref[:, pl.ds(0, k)] + there_ref[:, pl.ds(0, k)]).astype(BF16)
    padded[pl.ds(0, count), :] = jnp.zeros((count, k), BF16)
    padded[pl.ds(count, count), :] = picked
    ints = here_ref[:, pl.ds(k, LANES)] + there_ref[:, pl.ds(k, LANES)]
    schur = ints - dot_lanes(picked, padded[...])
    tile = (count, LANES)
    eye = jnp.where(iota(tile, 0) == iota(tile, 1), 1.0, 0.0)
    m_ref[...] = jnp.where(iota(tile, 1) < count, eye, schur)
    lower = halves(inverse_factor(m_ref, d_ref, count))

    icopy.wait()
    dcopy.wait()
    for j in range(most):
        vcopies[j].wait()
        prod = dot_lanes(vbuf[j], padded[...])
        start = pl.multiple_of(slots[j] * blk, blk)
        remain[:, pl.ds(j * blk, blk)] = ibuf[:, pl.ds(start, blk)] - prod.T[count:, :]
    upd_ref[...] = dbuf[...]
    high, low = halves(remain[...])
    cols = dot(lower[0], high) + dot(lower[0], low) + dot(lower[1], high)
    top = jnp.zeros((1, blk), F32)
    for j in range(most):
        s = slots[j]
        live = live_ref[s] > 0
        mine = cols[:, j * blk : (j + 1) * blk]
        left = dbuf[pl.ds(s, 1), :] - jnp.sum(mine * mine, axis=0, keepdims=True)
        left = jnp.where(iota((1, blk), 1) + s * blk == meta_ref[0], 0.0, left)
        cols_ref[:, pl.ds(pl.multiple_of(s * blk, blk), blk)] = jnp.where(live, mine, 0.0)
        upd_ref[pl.ds(s, 1), :] = jnp.where(live, left, dbuf[pl.ds(s, 1), :])
        top = jnp.maximum(top, jnp.where(live, left, 0.0))
    top_ref[...] = jnp.broadcast_to(top, top_ref.shape)


def step(here, there, vec, ict, diag, live, meta, copies):
    count, rows = ict.shape
    k = vec.shape[1]
    total = live.shape[0]
    blk = rows // total
    most = min(LIVE_MOST, total)
    return pl.pallas_call(
        step_kernel,
        out_shape=(
            jax.ShapeDtypeStruct((count, rows), F32),
            jax.ShapeDtypeStruct((total, blk), F32),
            jax.ShapeDtypeStruct((copies, blk), F32),
        ),
        in_specs=[VMEM, VMEM, ANY, ANY, ANY, SMEM, SMEM],
        out_specs=(VMEM, VMEM, VMEM),
        scratch_shapes=[
            pltpu.VMEM((most, blk, k), BF16),
            pltpu.VMEM((count, rows), F32),
            pltpu.VMEM((total, blk), F32),
            pltpu.VMEM((2 * count, k), BF16),
            pltpu.VMEM((count, LANES), F32),
            pltpu.VMEM((count, LANES), F32),
            pltpu.VMEM((count, most * blk), F32),
            pltpu.SMEM((total + 1,), jnp.int32),
            pltpu.SemaphoreType.DMA((most,)),
            pltpu.SemaphoreType.DMA((2,)),
        ],
        compiler_params=pltpu.CompilerParams(vmem_limit_bytes=24 << 20),
        name="step",
    )(here, there, vec, ict, diag, live, meta)


def scale_kernel(tops_ref, upd_ref, rel_ref, peak_ref):
    peak = jnp.max(jnp.max(tops_ref[...], axis=0, keepdims=True), axis=1, keepdims=True)
    rel_ref[...] = upd_ref[...] / peak
    peak_ref[...] = peak


def scale(tops, upd):
    return pl.pallas_call(
        scale_kernel,
        out_shape=(
            jax.ShapeDtypeStruct(upd.shape, F32),
            jax.ShapeDtypeStruct((1, 1), F32),
        ),
        in_specs=[VMEM, VMEM],
        out_specs=(VMEM, VMEM),
        compiler_params=pltpu.CompilerParams(vmem_limit_bytes=4 << 20),
        name="scale",
    )(tops, upd)


def exchange(blocks, axes):
    return lax.all_to_all(blocks, axes, split_axis=0, concat_axis=0, tiled=True)


def on_device(vec, ints, diag, spb, live, pivots):
    count = pivots.shape[0]
    ict = ints.T
    sizes = {a: lax.axis_size(a) for a in AXES}
    near = sizes["y"] * sizes["x"]
    mine, meta = pick(pivots[None, :], spb, vec, ict, sizes["z"])
    column = exchange(mine, "z")
    rows = exchange(jnp.broadcast_to(column, (near, *column.shape)), ("y", "x"))
    placed = place(rows.reshape(-1, rows.shape[-1]), count)
    other = lax.ppermute(placed, "c", [(0, 1), (1, 0)])
    cols, upd, top = step(
        placed, other, vec, ict, diag.reshape(live.shape[0], -1), live, meta, near * sizes["z"] * sizes["c"]
    )
    rel, peak = scale(exchange(top, AXES), upd)
    return (cols.T, rel.reshape(-1), peak.reshape(()))


def solution(mesh):
    split = Mesh(mesh.devices.reshape(8, 4, 2, mesh.shape["grp"]), AXES)
    in_specs = (P(AXES, None), P(AXES, None), P(AXES), P(AXES), P(AXES), P())
    out_specs = (P(AXES, None), P(AXES), P())
    return jax.shard_map(
        on_device, mesh=split, in_specs=in_specs, out_specs=out_specs, check_vma=False
    )
```

```python
import jax
import jax.numpy as jnp
from jax import lax
from jax.experimental import pallas as pl
from jax.experimental.pallas import tpu as pltpu
from jax.sharding import Mesh
from jax.sharding import PartitionSpec as P

AXES = ("z", "y", "c", "x")
LANES = 128
LIVE_MOST = 12
VMEM = pl.BlockSpec(memory_space=pltpu.VMEM)
SMEM = pl.BlockSpec(memory_space=pltpu.SMEM)
ANY = pl.BlockSpec(memory_space=pltpu.HBM)
F32 = jnp.float32
BF16 = jnp.bfloat16


def iota(shape, dim):
    return lax.broadcasted_iota(jnp.int32, shape, dim)


def in_hbm(a):
    return pltpu.with_memory_space_constraint(a, pltpu.HBM)


def dot_lanes(a, b, **kw):
    return lax.dot_general(a, b, (((1,), (1,)), ((), ())), preferred_element_type=F32, **kw)


def dot(a, b):
    return lax.dot_general(a, b, (((1,), (0,)), ((), ())), preferred_element_type=F32)


def halves(a):
    hi = a.astype(BF16)
    return hi, (a - hi.astype(F32)).astype(BF16)


def pick_kernel(count, piv_ref, spb_ref, vec_ref, ict_ref, out_ref, meta_ref, vbuf, ibuf, sems):
    piv = piv_ref[...]
    group, offset = piv >> 7, piv & (LANES - 1)
    code = jnp.zeros(piv.shape, jnp.int32)
    for s in range(spb_ref.shape[0]):
        code = jnp.where(
            group == spb_ref[s], (s * LANES + offset) * count + iota(piv.shape, 1) + 1, code
        )
    best = jnp.max(code.astype(F32)).astype(jnp.int32)
    has = best > 0
    at = jnp.maximum(best - 1, 0)
    row, q = at // count, at % count
    vcopy = pltpu.make_async_copy(
        vec_ref.at[pl.ds(pl.multiple_of((row // 8) * 8, 8), 8), :], vbuf, sems.at[0]
    )
    icopy = pltpu.make_async_copy(
        ict_ref.at[:, pl.ds(pl.multiple_of((row // LANES) * LANES, LANES), LANES)],
        ibuf.at[pl.ds(count, count), :],
        sems.at[1],
    )
    vcopy.start()
    icopy.start()
    meta_ref[0] = jnp.where(has, row, -1)
    ibuf[pl.ds(0, count), :] = jnp.zeros((count, LANES), F32)
    k = vbuf.shape[1]
    vcopy.wait()
    mine = (iota(vbuf.shape, 0) == row % 8) & has
    vrow = jnp.sum(jnp.where(mine, vbuf[...].astype(F32), 0.0), axis=0, keepdims=True)
    copies = out_ref.shape[0]
    for i in range(copies):
        out_ref[i, :, pl.ds(0, k)] = vrow
    icopy.wait()
    tile = (8, LANES)
    hot = jnp.where((iota(tile, 1) == row % LANES) & has, 1.0, 0.0)
    ints = dot_lanes(hot, ibuf[...], precision=lax.Precision.HIGHEST)
    index = jnp.where(has, q + 1, 0).astype(F32)
    tail = jnp.where(iota(tile, 1) == 0, index, ints)[0:1]
    for i in range(copies):
        out_ref[i, :, pl.ds(k, LANES)] = tail


def pick(pivots, spb, vec, ict, copies):
    count, k = pivots.shape[1], vec.shape[1]
    return pl.pallas_call(
        lambda *refs: pick_kernel(count, *refs),
        out_shape=(
            jax.ShapeDtypeStruct((copies, 1, k + LANES), F32),
            jax.ShapeDtypeStruct((1,), jnp.int32),
        ),
        in_specs=[VMEM, SMEM, ANY, ANY],
        out_specs=(VMEM, SMEM),
        scratch_shapes=[
            pltpu.VMEM((8, k), BF16),
            pltpu.VMEM((2 * count, LANES), F32),
            pltpu.SemaphoreType.DMA((2,)),
        ],
        compiler_params=pltpu.CompilerParams(vmem_limit_bytes=8 << 20),
        name="pick",
    )(in_hbm(pivots), in_hbm(spb), in_hbm(vec), in_hbm(ict))


def place_kernel(rows_ref, out_ref):
    k = rows_ref.shape[1] - LANES
    tail = rows_ref[:, pl.ds(k, LANES)]
    hot = tail[:, 0:1].astype(jnp.int32) - 1 == iota((rows_ref.shape[0], out_ref.shape[0]), 1)
    hot = jnp.where(hot, 1.0, 0.0).astype(BF16)
    turn = (((0,), (0,)), ((), ()))
    out_ref[:, pl.ds(0, k)] = lax.dot_general(
        hot, rows_ref[:, pl.ds(0, k)].astype(BF16), turn, preferred_element_type=F32
    )
    total = jnp.zeros((out_ref.shape[0], LANES), F32)
    for _ in range(3):
        part = tail.astype(BF16)
        tail = tail - part.astype(F32)
        total += lax.dot_general(hot, part, turn, preferred_element_type=F32)
    out_ref[:, pl.ds(k, LANES)] = total


def place(rows, count):
    return pl.pallas_call(
        place_kernel,
        out_shape=jax.ShapeDtypeStruct((count, rows.shape[1]), F32),
        in_specs=[VMEM],
        out_specs=VMEM,
        compiler_params=pltpu.CompilerParams(vmem_limit_bytes=8 << 20),
        name="place",
    )(rows)


def eliminate(blocks, at):
    n = len(blocks)
    lead = 8 * n + 8 * at
    tile = blocks[0].shape
    columns = [
        {i: jnp.broadcast_to(blocks[i][:, lead + j : lead + j + 1], tile) for i in range(at, n)}
        for j in range(8)
    ]
    pivot = jnp.ones(tile, F32)
    for j in range(8):
        row = jnp.broadcast_to(blocks[at][j : j + 1], tile)
        d = jnp.broadcast_to(columns[j][at][j : j + 1], tile)
        inverse = 1.0 / d
        pivot = jnp.where(iota(tile, 0) == j, d, pivot)
        across = [jnp.broadcast_to(columns[m][at][j : j + 1], tile) for m in range(j + 1, 8)]
        for i in range(at, n):
            by = columns[j][i] * inverse
            if i == at:
                by = jnp.where(iota(tile, 0) > j, by, 0.0)
            blocks[i] = blocks[i] - by * row
            for m in range(j + 1, 8):
                columns[m][i] = columns[m][i] - by * across[m - j - 1]
    return blocks[at] * lax.rsqrt(pivot)


def step_kernel(
    here_ref, there_ref, vec_ref, ict_ref, diag_ref, live_ref, meta_ref,
    cols_ref, upd_ref, top_ref,
    vbuf, padded, lower, remain, slots, vsems,
):
    most, blk, k = vbuf.shape
    count = here_ref.shape[0]
    total = live_ref.shape[0]
    found = jnp.int32(0)
    for s in range(total):
        slots[found] = s
        found += live_ref[s]
    for s in range(total):
        slots[found] = s
        found += 1 - live_ref[s]
    vcopies = []
    for j in range(most):
        start = pl.multiple_of(slots[j] * blk, blk)
        vcopies.append(
            pltpu.make_async_copy(vec_ref.at[pl.ds(start, blk), :], vbuf.at[j], vsems.at[j])
        )
        vcopies[-1].start()

    cols_ref[...] = jnp.zeros(cols_ref.shape, F32)
    picked = (here_ref[:, pl.ds(0, k)] + there_ref[:, pl.ds(0, k)]).astype(BF16)
    padded[pl.ds(0, count), :] = jnp.zeros((count, k), BF16)
    padded[pl.ds(count, count), :] = picked
    ints = here_ref[:, pl.ds(k, LANES)] + there_ref[:, pl.ds(k, LANES)]
    schur = ints - dot_lanes(picked, padded[...])
    tile = (count, LANES)
    eye = jnp.where(iota(tile, 0) == iota(tile, 1), 1.0, 0.0)
    whole = jnp.where(iota(tile, 1) < count, eye, schur)
    panels = count // 8
    blocks = [whole[8 * i : 8 * i + 8] for i in range(panels)]
    for at in range(panels):
        for j in range(most * at // panels, most * (at + 1) // panels):
            vcopies[j].wait()
            prod = dot_lanes(vbuf[j], padded[...])
            start = pl.multiple_of(slots[j] * blk, blk)
            remain[:, pl.ds(j * blk, blk)] = ict_ref[:, pl.ds(start, blk)] - prod.T[count:, :]
        lower[pl.ds(8 * at, 8), :] = eliminate(blocks, at)
    upd_ref[...] = diag_ref[...]
    high, low = halves(remain[...])
    lhigh, llow = halves(lower[:, pl.ds(0, count)])
    cols = dot(lhigh, high) + dot(lhigh, low) + dot(llow, high)
    top = jnp.zeros((1, blk), F32)
    for j in range(most):
        s = slots[j]
        live = live_ref[s] > 0
        mine = cols[:, j * blk : (j + 1) * blk]
        left = diag_ref[pl.ds(s, 1), :] - jnp.sum(mine * mine, axis=0, keepdims=True)
        left = jnp.where(iota((1, blk), 1) + s * blk == meta_ref[0], 0.0, left)
        cols_ref[:, pl.ds(pl.multiple_of(s * blk, blk), blk)] = jnp.where(live, mine, 0.0)
        upd_ref[pl.ds(s, 1), :] = jnp.where(live, left, diag_ref[pl.ds(s, 1), :])
        top = jnp.maximum(top, jnp.where(live, left, 0.0))
    top_ref[...] = jnp.broadcast_to(top, top_ref.shape)


def step(here, there, vec, ict, diag, live, meta, copies):
    count, rows = ict.shape
    k = vec.shape[1]
    total = live.shape[0]
    blk = rows // total
    most = min(LIVE_MOST, total)
    return pl.pallas_call(
        step_kernel,
        out_shape=(
            jax.ShapeDtypeStruct((count, rows), F32),
            jax.ShapeDtypeStruct((total, blk), F32),
            jax.ShapeDtypeStruct((copies, blk), F32),
        ),
        in_specs=[VMEM, VMEM, ANY, VMEM, VMEM, SMEM, SMEM],
        out_specs=(VMEM, VMEM, VMEM),
        scratch_shapes=[
            pltpu.VMEM((most, blk, k), BF16),
            pltpu.VMEM((2 * count, k), BF16),
            pltpu.VMEM((count, LANES), F32),
            pltpu.VMEM((count, most * blk), F32),
            pltpu.SMEM((total + 1,), jnp.int32),
            pltpu.SemaphoreType.DMA((most,)),
        ],
        compiler_params=pltpu.CompilerParams(vmem_limit_bytes=24 << 20),
        name="step",
    )(here, there, in_hbm(vec), ict, diag, live, meta)


def scale_kernel(tops_ref, upd_ref, rel_ref, peak_ref):
    peak = jnp.max(jnp.max(tops_ref[...], axis=0, keepdims=True), axis=1, keepdims=True)
    rel_ref[...] = upd_ref[...] / peak
    peak_ref[...] = peak


def scale(tops, upd):
    return pl.pallas_call(
        scale_kernel,
        out_shape=(
            jax.ShapeDtypeStruct(upd.shape, F32),
            jax.ShapeDtypeStruct((1, 1), F32),
        ),
        in_specs=[VMEM, VMEM],
        out_specs=(VMEM, VMEM),
        compiler_params=pltpu.CompilerParams(vmem_limit_bytes=4 << 20),
        name="scale",
    )(tops, upd)


def exchange(blocks, axes):
    return lax.all_to_all(blocks, axes, split_axis=0, concat_axis=0, tiled=True)


def on_device(vec, ints, diag, spb, live, pivots):
    count = pivots.shape[0]
    ict = ints.T
    sizes = {a: lax.axis_size(a) for a in AXES}
    near = sizes["y"] * sizes["x"]
    mine, meta = pick(pivots[None, :], spb, vec, ict, sizes["z"])
    column = exchange(mine, "z")
    column = column.reshape(column.shape[0], -1)
    rows = exchange(jnp.broadcast_to(column, (near, *column.shape)), ("y", "x"))
    placed = place(rows.reshape(-1, rows.shape[-1]), count)
    other = lax.ppermute(placed, "c", [(0, 1), (1, 0)])
    cols, upd, top = step(
        placed, other, vec, ict, diag.reshape(live.shape[0], -1), live, meta, near * sizes["z"] * sizes["c"]
    )
    rel, peak = scale(exchange(top, AXES), upd)
    return (cols.T, rel.reshape(-1), peak.reshape(()))


def solution(mesh):
    split = Mesh(mesh.devices.reshape(8, 4, 2, mesh.shape["grp"]), AXES)
    in_specs = (P(AXES, None), P(AXES, None), P(AXES), P(AXES), P(AXES), P())
    out_specs = (P(AXES, None), P(AXES), P())
    return jax.shard_map(
        on_device, mesh=split, in_specs=in_specs, out_specs=out_specs, check_vma=False
    )
```

```python
import jax
import jax.numpy as jnp
from jax import lax
from jax.experimental import pallas as pl
from jax.experimental.pallas import tpu as pltpu
from jax.sharding import Mesh
from jax.sharding import PartitionSpec as P

AXES = ("z", "y", "c", "x")
LANES = 128
LIVE_MOST = 12
VMEM = pl.BlockSpec(memory_space=pltpu.VMEM)
SMEM = pl.BlockSpec(memory_space=pltpu.SMEM)
ANY = pl.BlockSpec(memory_space=pltpu.HBM)
F32 = jnp.float32
BF16 = jnp.bfloat16


def iota(shape, dim):
    return lax.broadcasted_iota(jnp.int32, shape, dim)


def in_hbm(a):
    return pltpu.with_memory_space_constraint(a, pltpu.HBM)


def dot_lanes(a, b, **kw):
    return lax.dot_general(a, b, (((1,), (1,)), ((), ())), preferred_element_type=F32, **kw)


def dot(a, b):
    return lax.dot_general(a, b, (((1,), (0,)), ((), ())), preferred_element_type=F32)


def halves(a):
    hi = a.astype(BF16)
    return hi, (a - hi.astype(F32)).astype(BF16)


def pick_kernel(count, piv_ref, spb_ref, vec_ref, ict_ref, out_ref, meta_ref, vbuf, ibuf, sems):
    piv = piv_ref[...]
    group, offset = piv >> 7, piv & (LANES - 1)
    code = jnp.zeros(piv.shape, jnp.int32)
    for s in range(spb_ref.shape[0]):
        code = jnp.where(
            group == spb_ref[s], (s * LANES + offset) * count + iota(piv.shape, 1) + 1, code
        )
    best = jnp.max(code.astype(F32)).astype(jnp.int32)
    has = best > 0
    at = jnp.maximum(best - 1, 0)
    row, q = at // count, at % count
    vcopy = pltpu.make_async_copy(
        vec_ref.at[pl.ds(pl.multiple_of((row // 8) * 8, 8), 8), :], vbuf, sems.at[0]
    )
    icopy = pltpu.make_async_copy(
        ict_ref.at[:, pl.ds(pl.multiple_of((row // LANES) * LANES, LANES), LANES)],
        ibuf.at[pl.ds(count, count), :],
        sems.at[1],
    )
    vcopy.start()
    icopy.start()
    meta_ref[0] = jnp.where(has, row, -1)
    ibuf[pl.ds(0, count), :] = jnp.zeros((count, LANES), F32)
    k = vbuf.shape[1]
    vcopy.wait()
    mine = (iota(vbuf.shape, 0) == row % 8) & has
    vrow = jnp.sum(jnp.where(mine, vbuf[...].astype(F32), 0.0), axis=0, keepdims=True)
    copies = out_ref.shape[0]
    for i in range(copies):
        out_ref[i, :, pl.ds(0, k)] = vrow
    icopy.wait()
    tile = (8, LANES)
    hot = jnp.where((iota(tile, 1) == row % LANES) & has, 1.0, 0.0)
    ints = dot_lanes(hot, ibuf[...], precision=lax.Precision.HIGHEST)
    index = jnp.where(has, q + 1, 0).astype(F32)
    tail = jnp.where(iota(tile, 1) == 0, index, ints)[0:1]
    for i in range(copies):
        out_ref[i, :, pl.ds(k, LANES)] = tail


def pick(pivots, spb, vec, ict, copies):
    count, k = pivots.shape[1], vec.shape[1]
    return pl.pallas_call(
        lambda *refs: pick_kernel(count, *refs),
        out_shape=(
            jax.ShapeDtypeStruct((copies, 1, k + LANES), F32),
            jax.ShapeDtypeStruct((1,), jnp.int32),
        ),
        in_specs=[VMEM, SMEM, ANY, ANY],
        out_specs=(VMEM, SMEM),
        scratch_shapes=[
            pltpu.VMEM((8, k), BF16),
            pltpu.VMEM((2 * count, LANES), F32),
            pltpu.SemaphoreType.DMA((2,)),
        ],
        compiler_params=pltpu.CompilerParams(vmem_limit_bytes=8 << 20),
        name="pick",
    )(in_hbm(pivots), in_hbm(spb), in_hbm(vec), in_hbm(ict))


def place_kernel(rows_ref, out_ref):
    k = rows_ref.shape[1] - LANES
    tail = rows_ref[:, pl.ds(k, LANES)]
    hot = tail[:, 0:1].astype(jnp.int32) - 1 == iota((rows_ref.shape[0], out_ref.shape[0]), 1)
    hot = jnp.where(hot, 1.0, 0.0).astype(BF16)
    turn = (((0,), (0,)), ((), ()))
    out_ref[:, pl.ds(0, k)] = lax.dot_general(
        hot, rows_ref[:, pl.ds(0, k)].astype(BF16), turn, preferred_element_type=F32
    )
    total = jnp.zeros((out_ref.shape[0], LANES), F32)
    for _ in range(3):
        part = tail.astype(BF16)
        tail = tail - part.astype(F32)
        total += lax.dot_general(hot, part, turn, preferred_element_type=F32)
    out_ref[:, pl.ds(k, LANES)] = total


def place(rows, count):
    return pl.pallas_call(
        place_kernel,
        out_shape=jax.ShapeDtypeStruct((count, rows.shape[1]), F32),
        in_specs=[VMEM],
        out_specs=VMEM,
        compiler_params=pltpu.CompilerParams(vmem_limit_bytes=8 << 20),
        name="place",
    )(rows)


def eliminate(blocks, at):
    n = len(blocks)
    lead = 8 * n + 8 * at
    tile = blocks[0].shape
    columns = [
        {i: jnp.broadcast_to(blocks[i][:, lead + j : lead + j + 1], tile) for i in range(at, n)}
        for j in range(8)
    ]
    pivot = jnp.ones(tile, F32)
    for j in range(8):
        row = jnp.broadcast_to(blocks[at][j : j + 1], tile)
        d = jnp.broadcast_to(columns[j][at][j : j + 1], tile)
        inverse = 1.0 / d
        pivot = jnp.where(iota(tile, 0) == j, d, pivot)
        across = [jnp.broadcast_to(columns[m][at][j : j + 1], tile) for m in range(j + 1, 8)]
        for i in range(at, n):
            by = columns[j][i] * inverse
            if i == at:
                by = jnp.where(iota(tile, 0) > j, by, 0.0)
            blocks[i] = blocks[i] - by * row
            for m in range(j + 1, 8):
                columns[m][i] = columns[m][i] - by * across[m - j - 1]
    return blocks[at] * lax.rsqrt(pivot)


def step_kernel(
    here_ref, there_ref, vec_ref, ict_ref, diag_ref, live_ref, meta_ref,
    cols_ref, upd_ref, top_ref,
    padded, lower, remain, slots,
):
    count, total = here_ref.shape[0], live_ref.shape[0]
    k = vec_ref.shape[1]
    blk = vec_ref.shape[0] // total
    most = remain.shape[1] // blk
    found = jnp.int32(0)
    for s in range(total):
        slots[found] = s
        found += live_ref[s]
    for s in range(total):
        slots[found] = s
        found += 1 - live_ref[s]
    cols_ref[...] = jnp.zeros(cols_ref.shape, F32)
    picked = (here_ref[:, pl.ds(0, k)] + there_ref[:, pl.ds(0, k)]).astype(BF16)
    padded[pl.ds(0, count), :] = jnp.zeros((count, k), BF16)
    padded[pl.ds(count, count), :] = picked
    ints = here_ref[:, pl.ds(k, LANES)] + there_ref[:, pl.ds(k, LANES)]
    schur = ints - dot_lanes(picked, padded[...])
    tile = (count, LANES)
    eye = jnp.where(iota(tile, 0) == iota(tile, 1), 1.0, 0.0)
    whole = jnp.where(iota(tile, 1) < count, eye, schur)
    panels = count // 8
    blocks = [whole[8 * i : 8 * i + 8] for i in range(panels)]
    chunk = 4
    places = [1, 3, 5]
    for at in range(panels):
        for first in [chunk * c for c, p in enumerate(places) if p == at]:
            starts = [pl.multiple_of(slots[first + j] * blk, blk) for j in range(chunk)]
            part = jnp.concatenate([vec_ref[pl.ds(start, blk), :] for start in starts])
            prod = dot_lanes(picked, part)
            for j, start in enumerate(starts):
                remain[:, pl.ds((first + j) * blk, blk)] = (
                    ict_ref[:, pl.ds(start, blk)] - prod[:, j * blk : (j + 1) * blk]
                )
        lower[pl.ds(8 * at, 8), :] = eliminate(blocks, at)
    upd_ref[...] = diag_ref[...]
    high, low = halves(remain[...])
    lhigh, llow = halves(lower[:, pl.ds(0, count)])
    cols = dot(lhigh, high) + dot(lhigh, low) + dot(llow, high)
    top = jnp.zeros((1, blk), F32)
    for j in range(most):
        s = slots[j]
        live = live_ref[s] > 0
        mine = cols[:, j * blk : (j + 1) * blk]
        left = diag_ref[pl.ds(s, 1), :] - jnp.sum(mine * mine, axis=0, keepdims=True)
        left = jnp.where(iota((1, blk), 1) + s * blk == meta_ref[0], 0.0, left)
        cols_ref[:, pl.ds(pl.multiple_of(s * blk, blk), blk)] = jnp.where(live, mine, 0.0)
        upd_ref[pl.ds(s, 1), :] = jnp.where(live, left, diag_ref[pl.ds(s, 1), :])
        top = jnp.maximum(top, jnp.where(live, left, 0.0))
    top_ref[...] = jnp.broadcast_to(top, top_ref.shape)


def step(here, there, vec, ict, diag, live, meta, copies):
    count, rows = ict.shape
    k = vec.shape[1]
    total = live.shape[0]
    blk = rows // total
    most = min(LIVE_MOST, total)
    return pl.pallas_call(
        step_kernel,
        out_shape=(
            jax.ShapeDtypeStruct((count, rows), F32),
            jax.ShapeDtypeStruct((total, blk), F32),
            jax.ShapeDtypeStruct((copies, blk), F32),
        ),
        in_specs=[VMEM, VMEM, VMEM, VMEM, VMEM, SMEM, SMEM],
        out_specs=(VMEM, VMEM, VMEM),
        scratch_shapes=[
            pltpu.VMEM((2 * count, k), BF16),
            pltpu.VMEM((count, LANES), F32),
            pltpu.VMEM((count, most * blk), F32),
            pltpu.SMEM((total + 1,), jnp.int32),
        ],
        compiler_params=pltpu.CompilerParams(vmem_limit_bytes=24 << 20),
        name="step",
    )(here, there, vec, ict, diag, live, meta)


def scale_kernel(tops_ref, upd_ref, rel_ref, peak_ref):
    peak = jnp.max(jnp.max(tops_ref[...], axis=0, keepdims=True), axis=1, keepdims=True)
    rel_ref[...] = upd_ref[...] / peak
    peak_ref[...] = peak


def scale(tops, upd):
    return pl.pallas_call(
        scale_kernel,
        out_shape=(
            jax.ShapeDtypeStruct(upd.shape, F32),
            jax.ShapeDtypeStruct((1, 1), F32),
        ),
        in_specs=[VMEM, VMEM],
        out_specs=(VMEM, VMEM),
        compiler_params=pltpu.CompilerParams(vmem_limit_bytes=4 << 20),
        name="scale",
    )(tops, upd)


def exchange(blocks, axes):
    return lax.all_to_all(blocks, axes, split_axis=0, concat_axis=0, tiled=True)


def on_device(vec, ints, diag, spb, live, pivots):
    count = pivots.shape[0]
    ict = ints.T
    sizes = {a: lax.axis_size(a) for a in AXES}
    near = sizes["y"] * sizes["x"]
    mine, meta = pick(pivots[None, :], spb, vec, ict, sizes["z"])
    column = exchange(mine, "z")
    column = column.reshape(column.shape[0], -1)
    rows = exchange(jnp.broadcast_to(column, (near, *column.shape)), ("y", "x"))
    placed = place(rows.reshape(-1, rows.shape[-1]), count)
    other = lax.ppermute(placed, "c", [(0, 1), (1, 0)])
    cols, upd, top = step(
        placed, other, vec, ict, diag.reshape(live.shape[0], -1), live, meta, near * sizes["z"] * sizes["c"]
    )
    rel, peak = scale(exchange(top, AXES), upd)
    return (cols.T, rel.reshape(-1), peak.reshape(()))


def solution(mesh):
    split = Mesh(mesh.devices.reshape(8, 4, 2, mesh.shape["grp"]), AXES)
    in_specs = (P(AXES, None), P(AXES, None), P(AXES), P(AXES), P(AXES), P())
    out_specs = (P(AXES, None), P(AXES), P())
    return jax.shard_map(
        on_device, mesh=split, in_specs=in_specs, out_specs=out_specs, check_vma=False
    )
```

```python
import functools
import math

import jax
import jax.numpy as jnp
import numpy as np
from jax import lax
from jax.experimental import pallas as pl
from jax.experimental.pallas import tpu as pltpu
from jax.sharding import Mesh
from jax.sharding import PartitionSpec as P

AXES = ("z", "y", "c", "x")
LANES = 128
LIVE_MOST = 12
VMEM = pl.BlockSpec(memory_space=pltpu.VMEM)
SMEM = pl.BlockSpec(memory_space=pltpu.SMEM)
ANY = pl.BlockSpec(memory_space=pltpu.HBM)
F32 = jnp.float32
BF16 = jnp.bfloat16


def iota(shape, dim):
    return lax.broadcasted_iota(jnp.int32, shape, dim)


def in_hbm(a):
    return pltpu.with_memory_space_constraint(a, pltpu.HBM)


def dot_lanes(a, b, **kw):
    return lax.dot_general(a, b, (((1,), (1,)), ((), ())), preferred_element_type=F32, **kw)


def dot(a, b):
    return lax.dot_general(a, b, (((1,), (0,)), ((), ())), preferred_element_type=F32)


def halves(a):
    hi = a.astype(BF16)
    return hi, (a - hi.astype(F32)).astype(BF16)


def pick_kernel(
    count, piv_ref, spb_ref, live_ref, vec_ref, ict_ref, out_ref, plan_ref, vbuf, ibuf, sems
):
    piv = piv_ref[...]
    group, offset = piv >> 7, piv & (LANES - 1)
    code = jnp.zeros(piv.shape, jnp.int32)
    for s in range(spb_ref.shape[0]):
        code = jnp.where(
            group == spb_ref[s], (s * LANES + offset) * count + iota(piv.shape, 1) + 1, code
        )
    best = jnp.max(code.astype(F32)).astype(jnp.int32)
    has = best > 0
    at = jnp.maximum(best - 1, 0)
    row, q = at // count, at % count
    vcopy = pltpu.make_async_copy(
        vec_ref.at[pl.ds(pl.multiple_of((row // 8) * 8, 8), 8), :], vbuf, sems.at[0]
    )
    icopy = pltpu.make_async_copy(
        ict_ref.at[:, pl.ds(pl.multiple_of((row // LANES) * LANES, LANES), LANES)],
        ibuf.at[pl.ds(count, count), :],
        sems.at[1],
    )
    vcopy.start()
    icopy.start()
    total = live_ref.shape[0]
    found = jnp.int32(0)
    for wanted in (1, 0):
        for s in range(total):
            plan_ref[found] = s
            plan_ref[total + found] = wanted
            found += (live_ref[s] > 0) == (wanted > 0)
    plan_ref[2 * total] = jnp.where(has, row, -1)
    ibuf[pl.ds(0, count), :] = jnp.zeros((count, LANES), F32)
    k = vbuf.shape[1]
    vcopy.wait()
    mine = (iota(vbuf.shape, 0) == row % 8) & has
    vrow = jnp.sum(jnp.where(mine, vbuf[...].astype(F32), 0.0), axis=0, keepdims=True)
    copies = out_ref.shape[0]
    for i in range(copies):
        out_ref[i, :, pl.ds(0, k)] = vrow
    icopy.wait()
    tile = (8, LANES)
    hot = jnp.where((iota(tile, 1) == row % LANES) & has, 1.0, 0.0)
    ints = dot_lanes(hot, ibuf[...], precision=lax.Precision.HIGHEST)
    index = jnp.where(has, q + 1, 0).astype(F32)
    tail = jnp.where(iota(tile, 1) == 0, index, ints)[0:1]
    for i in range(copies):
        out_ref[i, :, pl.ds(k, LANES)] = tail


def pick(pivots, spb, live, vec, ict, copies):
    count, k = pivots.shape[1], vec.shape[1]
    return pl.pallas_call(
        lambda *refs: pick_kernel(count, *refs),
        out_shape=(
            jax.ShapeDtypeStruct((copies, 1, k + LANES), F32),
            pltpu.SMEM((2 * live.shape[0] + 2,), jnp.int32),
        ),
        in_specs=[VMEM, SMEM, SMEM, ANY, ANY],
        out_specs=(VMEM, SMEM),
        scratch_shapes=[
            pltpu.VMEM((8, k), BF16),
            pltpu.VMEM((2 * count, LANES), F32),
            pltpu.SemaphoreType.DMA((2,)),
        ],
        compiler_params=pltpu.CompilerParams(vmem_limit_bytes=8 << 20),
        name="pick",
    )(in_hbm(pivots), in_hbm(spb), in_hbm(live), in_hbm(vec), in_hbm(ict))


def place_kernel(rows_ref, out_ref):
    k = rows_ref.shape[1] - LANES
    tail = rows_ref[:, pl.ds(k, LANES)]
    hot = tail[:, 0:1].astype(jnp.int32) - 1 == iota((rows_ref.shape[0], out_ref.shape[0]), 1)
    hot = jnp.where(hot, 1.0, 0.0).astype(BF16)
    turn = (((0,), (0,)), ((), ()))
    out_ref[:, pl.ds(0, k)] = lax.dot_general(
        hot, rows_ref[:, pl.ds(0, k)].astype(BF16), turn, preferred_element_type=F32
    )
    total = jnp.zeros((out_ref.shape[0], LANES), F32)
    for _ in range(3):
        part = tail.astype(BF16)
        tail = tail - part.astype(F32)
        total += lax.dot_general(hot, part, turn, preferred_element_type=F32)
    out_ref[:, pl.ds(k, LANES)] = total


def place(rows, count):
    return pl.pallas_call(
        place_kernel,
        out_shape=jax.ShapeDtypeStruct((count, rows.shape[1]), F32),
        in_specs=[VMEM],
        out_specs=VMEM,
        compiler_params=pltpu.CompilerParams(vmem_limit_bytes=8 << 20),
        name="place",
    )(rows)


def eliminate(blocks, at):
    n = len(blocks)
    lead = 8 * n + 8 * at
    tile = blocks[0].shape
    columns = [
        {i: jnp.broadcast_to(blocks[i][:, lead + j : lead + j + 1], tile) for i in range(at, n)}
        for j in range(8)
    ]
    pivot = jnp.ones(tile, F32)
    for j in range(8):
        row = jnp.broadcast_to(blocks[at][j : j + 1], tile)
        d = jnp.broadcast_to(columns[j][at][j : j + 1], tile)
        inverse = 1.0 / d
        pivot = jnp.where(iota(tile, 0) == j, d, pivot)
        across = [jnp.broadcast_to(columns[m][at][j : j + 1], tile) for m in range(j + 1, 8)]
        for i in range(at, n):
            by = columns[j][i] * inverse
            if i == at:
                by = jnp.where(iota(tile, 0) > j, by, 0.0)
            blocks[i] = blocks[i] - by * row
            for m in range(j + 1, 8):
                columns[m][i] = columns[m][i] - by * across[m - j - 1]
    return blocks[at] * lax.rsqrt(pivot)


def step_kernel(
    here_ref, there_ref, vec_ref, ict_ref, diag_ref, plan_ref,
    cols_ref, upd_ref, top_ref,
    padded, lower, remain,
):
    count, total = here_ref.shape[0], diag_ref.shape[0]
    k = vec_ref.shape[1]
    blk = vec_ref.shape[0] // total
    most = remain.shape[1] // blk
    cols_ref[...] = jnp.zeros(cols_ref.shape, F32)
    picked = (here_ref[:, pl.ds(0, k)] + there_ref[:, pl.ds(0, k)]).astype(BF16)
    padded[pl.ds(0, count), :] = jnp.zeros((count, k), BF16)
    padded[pl.ds(count, count), :] = picked
    ints = here_ref[:, pl.ds(k, LANES)] + there_ref[:, pl.ds(k, LANES)]
    schur = ints - dot_lanes(picked, padded[...])
    tile = (count, LANES)
    eye = jnp.where(iota(tile, 0) == iota(tile, 1), 1.0, 0.0)
    whole = jnp.where(iota(tile, 1) < count, eye, schur)
    panels = count // 8
    blocks = [whole[8 * i : 8 * i + 8] for i in range(panels)]
    chunk = 4
    places = [0, 1, 2]
    for at in range(panels):
        for first in [chunk * c for c, p in enumerate(places) if p == at]:
            starts = [pl.multiple_of(plan_ref[first + j] * blk, blk) for j in range(chunk)]
            part = jnp.concatenate([vec_ref[pl.ds(start, blk), :] for start in starts])
            prod = dot_lanes(picked, part)
            for j, start in enumerate(starts):
                remain[:, pl.ds((first + j) * blk, blk)] = (
                    ict_ref[:, pl.ds(start, blk)] - prod[:, j * blk : (j + 1) * blk]
                )
        lower[pl.ds(8 * at, 8), :] = eliminate(blocks, at)
    upd_ref[...] = diag_ref[...]
    high, low = halves(remain[...])
    lhigh, llow = halves(lower[:, pl.ds(0, count)])
    cols = dot(lhigh, high) + dot(lhigh, low) + dot(llow, high)
    top = jnp.zeros((1, blk), F32)
    for j in range(most):
        s = plan_ref[j]
        live = plan_ref[total + j] > 0
        mine = cols[:, j * blk : (j + 1) * blk]
        left = diag_ref[pl.ds(s, 1), :] - jnp.sum(mine * mine, axis=0, keepdims=True)
        left = jnp.where(iota((1, blk), 1) + s * blk == plan_ref[2 * total], 0.0, left)
        cols_ref[:, pl.ds(pl.multiple_of(s * blk, blk), blk)] = jnp.where(live, mine, 0.0)
        upd_ref[pl.ds(s, 1), :] = jnp.where(live, left, diag_ref[pl.ds(s, 1), :])
        top = jnp.maximum(top, jnp.where(live, left, 0.0))
    top_ref[...] = jnp.broadcast_to(top, top_ref.shape)


def step(here, there, vec, ict, diag, plan, copies):
    count, rows = ict.shape
    k = vec.shape[1]
    total = diag.shape[0]
    blk = rows // total
    most = min(LIVE_MOST, total)
    return pl.pallas_call(
        step_kernel,
        out_shape=(
            pltpu.VMEM((count, rows), F32),
            pltpu.VMEM((total, blk), F32),
            pltpu.VMEM((copies, blk), F32),
        ),
        in_specs=[VMEM, VMEM, VMEM, VMEM, VMEM, SMEM],
        out_specs=(VMEM, VMEM, VMEM),
        scratch_shapes=[
            pltpu.VMEM((2 * count, k), BF16),
            pltpu.VMEM((count, LANES), F32),
            pltpu.VMEM((count, most * blk), F32),
        ],
        compiler_params=pltpu.CompilerParams(vmem_limit_bytes=24 << 20),
        name="step",
    )(here, there, vec, ict, diag, plan)


def scale_kernel(tops_ref, upd_ref, held_ref, cols_ref, rel_ref, peak_ref, sem):
    leaving = pltpu.make_async_copy(held_ref, cols_ref, sem)
    leaving.start()
    peak = jnp.max(jnp.max(tops_ref[...], axis=0, keepdims=True), axis=1, keepdims=True)
    rel_ref[...] = upd_ref[...] / peak
    peak_ref[...] = peak
    leaving.wait()


def scale(tops, upd, cols):
    return pl.pallas_call(
        scale_kernel,
        out_shape=(
            jax.ShapeDtypeStruct(cols.shape, F32),
            jax.ShapeDtypeStruct(upd.shape, F32),
            jax.ShapeDtypeStruct((1, 1), F32),
        ),
        in_specs=[VMEM, VMEM, VMEM],
        out_specs=(ANY, VMEM, VMEM),
        scratch_shapes=[pltpu.SemaphoreType.DMA],
        compiler_params=pltpu.CompilerParams(vmem_limit_bytes=4 << 20),
        name="scale",
    )(tops, upd, cols)


def exchange(blocks, groups=None):
    return lax.all_to_all(
        blocks, "d", split_axis=0, concat_axis=0, axis_index_groups=groups, tiled=True
    )


def on_device(shape, vec, ints, diag, spb, live, pivots):
    count = pivots.shape[0]
    ict = ints.T
    at = np.arange(math.prod(shape)).reshape(shape)
    wide = [at[:, :, 0, x].ravel().tolist() for x in range(shape[3])]
    wide += [at[:, y, 1, :].ravel().tolist() for y in range(shape[1])]
    near = [at[z, y, 0, :].tolist() for z in range(shape[0]) for y in range(shape[1])]
    near += [at[z, :, 1, x].tolist() for z in range(shape[0]) for x in range(shape[3])]
    mine, plan = pick(pivots[None, :], spb, live, vec, ict, len(wide[0]))
    sheet = exchange(mine, wide).reshape(len(wide[0]), -1)
    rows = exchange(jnp.broadcast_to(sheet, (len(near[0]), *sheet.shape)), near)
    placed = place(rows.reshape(-1, rows.shape[-1]), count)
    pairs = [(int(p), int(q)) for p, q in zip(at.ravel(), at[:, :, ::-1].ravel())]
    other = lax.ppermute(placed, "d", pairs)
    cols, upd, top = step(
        placed, other, vec, ict, diag.reshape(live.shape[0], -1), plan, at.size
    )
    cols, rel, peak = scale(exchange(top), upd, cols)
    return (cols.T, rel.reshape(-1), peak.reshape(()))


def solution(mesh):
    shape = (8, 4, 2, mesh.shape["grp"])
    flat = Mesh(mesh.devices.reshape(-1), ("d",))
    d = P("d")
    return jax.shard_map(
        functools.partial(on_device, shape),
        mesh=flat,
        in_specs=(d, d, d, d, d, P()),
        out_specs=(d, d, P()),
        check_vma=False,
    )
```

```python
import functools
import math

import jax
import jax.numpy as jnp
import numpy as np
from jax import lax
from jax.experimental import pallas as pl
from jax.experimental.pallas import tpu as pltpu
from jax.sharding import Mesh
from jax.sharding import PartitionSpec as P

AXES = ("z", "y", "c", "x")
LANES = 128
LIVE_MOST = 12
VMEM = pl.BlockSpec(memory_space=pltpu.VMEM)
SMEM = pl.BlockSpec(memory_space=pltpu.SMEM)
ANY = pl.BlockSpec(memory_space=pltpu.HBM)
F32 = jnp.float32
BF16 = jnp.bfloat16


def iota(shape, dim):
    return lax.broadcasted_iota(jnp.int32, shape, dim)


def in_hbm(a):
    return pltpu.with_memory_space_constraint(a, pltpu.HBM)


def dot_lanes(a, b):
    return lax.dot_general(a, b, (((1,), (1,)), ((), ())), preferred_element_type=F32)


def dot(a, b):
    return lax.dot_general(a, b, (((1,), (0,)), ((), ())), preferred_element_type=F32)


def halves(a):
    hi = a.astype(BF16)
    return hi, (a - hi.astype(F32)).astype(BF16)


def pick_kernel(
    count, piv_ref, spb_ref, live_ref, vec_ref, ict_ref, out_ref, plan_ref, vbuf, ibuf, sems
):
    piv = piv_ref[...]
    group, offset = piv >> 7, piv & (LANES - 1)
    code = jnp.zeros(piv.shape, jnp.int32)
    for s in range(spb_ref.shape[0]):
        code = jnp.where(
            group == spb_ref[s], (s * LANES + offset) * count + iota(piv.shape, 1) + 1, code
        )
    best = jnp.max(code.astype(F32)).astype(jnp.int32)
    has = best > 0
    at = jnp.maximum(best - 1, 0)
    row, q = at // count, at % count
    vcopy = pltpu.make_async_copy(
        vec_ref.at[pl.ds(pl.multiple_of((row // 8) * 8, 8), 8), :], vbuf, sems.at[0]
    )
    icopy = pltpu.make_async_copy(
        ict_ref.at[:, pl.ds(pl.multiple_of((row // LANES) * LANES, LANES), LANES)],
        ibuf.at[pl.ds(count, count), :],
        sems.at[1],
    )
    vcopy.start()
    icopy.start()
    total = live_ref.shape[0]
    found = jnp.int32(0)
    for wanted in (1, 0):
        for s in range(total):
            plan_ref[found] = s
            plan_ref[total + found] = wanted
            found += (live_ref[s] > 0) == (wanted > 0)
    plan_ref[2 * total] = jnp.where(has, row, -1)
    ibuf[pl.ds(0, count), :] = jnp.zeros((count, LANES), F32)
    k = vbuf.shape[1]
    vcopy.wait()
    mine = (iota(vbuf.shape, 0) == row % 8) & has
    vrow = jnp.sum(jnp.where(mine, vbuf[...].astype(F32), 0.0), axis=0, keepdims=True)
    copies = out_ref.shape[0]
    for i in range(copies):
        out_ref[i, :, pl.ds(0, k)] = vrow
    icopy.wait()
    tile = (8, LANES)
    hot = jnp.where((iota(tile, 1) == row % LANES) & has, 1.0, 0.0).astype(BF16)
    rest, ints = ibuf[...], jnp.zeros(tile, F32)
    for _ in range(3):
        part = rest.astype(BF16)
        rest = rest - part.astype(F32)
        ints += dot_lanes(hot, part)
    index = jnp.where(has, q + 1, 0).astype(F32)
    tail = jnp.where(iota(tile, 1) == 0, index, ints)[0:1]
    for i in range(copies):
        out_ref[i, :, pl.ds(k, LANES)] = tail


def pick(pivots, spb, live, vec, ict, copies):
    count, k = pivots.shape[1], vec.shape[1]
    return pl.pallas_call(
        lambda *refs: pick_kernel(count, *refs),
        out_shape=(
            jax.ShapeDtypeStruct((copies, 1, k + LANES), F32),
            pltpu.SMEM((2 * live.shape[0] + 2,), jnp.int32),
        ),
        in_specs=[VMEM, SMEM, SMEM, ANY, ANY],
        out_specs=(VMEM, SMEM),
        scratch_shapes=[
            pltpu.VMEM((8, k), BF16),
            pltpu.VMEM((2 * count, LANES), F32),
            pltpu.SemaphoreType.DMA((2,)),
        ],
        compiler_params=pltpu.CompilerParams(vmem_limit_bytes=8 << 20),
        name="pick",
    )(in_hbm(pivots), in_hbm(spb), in_hbm(live), in_hbm(vec), in_hbm(ict))


def place_kernel(*refs):
    *sheets, out_ref = refs
    k = out_ref.shape[1] - LANES
    turn = (((0,), (0,)), ((), ()))
    total = jnp.zeros((out_ref.shape[0], LANES), F32)
    hots = []
    tails = []
    for ref in sheets:
        tail = ref[:, pl.ds(k, LANES)]
        hot = tail[:, 0:1].astype(jnp.int32) - 1 == iota((ref.shape[0], out_ref.shape[0]), 1)
        hots.append(jnp.where(hot, 1.0, 0.0).astype(BF16))
        tails.append(tail)
    hot, tail = jnp.concatenate(hots), jnp.concatenate(tails)
    body = jnp.concatenate([ref[:, pl.ds(0, k)].astype(BF16) for ref in sheets])
    out_ref[:, pl.ds(0, k)] = lax.dot_general(hot, body, turn, preferred_element_type=F32)
    for _ in range(3):
        part = tail.astype(BF16)
        tail = tail - part.astype(F32)
        total += lax.dot_general(hot, part, turn, preferred_element_type=F32)
    out_ref[:, pl.ds(k, LANES)] = total


def place(sheets, count):
    return pl.pallas_call(
        place_kernel,
        out_shape=jax.ShapeDtypeStruct((count, sheets[0].shape[1]), F32),
        in_specs=[VMEM] * len(sheets),
        out_specs=VMEM,
        compiler_params=pltpu.CompilerParams(vmem_limit_bytes=8 << 20),
        name="place",
    )(*sheets)


def eliminate(blocks, at):
    n = len(blocks)
    lead = 8 * n + 8 * at
    tile = blocks[0].shape
    columns = [
        {i: jnp.broadcast_to(blocks[i][:, lead + j : lead + j + 1], tile) for i in range(at, n)}
        for j in range(8)
    ]
    pivot = jnp.ones(tile, F32)
    for j in range(8):
        row = jnp.broadcast_to(blocks[at][j : j + 1], tile)
        d = jnp.broadcast_to(columns[j][at][j : j + 1], tile)
        inverse = 1.0 / d
        pivot = jnp.where(iota(tile, 0) == j, d, pivot)
        across = [jnp.broadcast_to(columns[m][at][j : j + 1], tile) for m in range(j + 1, 8)]
        for i in range(at, n):
            by = columns[j][i] * inverse
            if i == at:
                by = jnp.where(iota(tile, 0) > j, by, 0.0)
            blocks[i] = blocks[i] - by * row
            for m in range(j + 1, 8):
                columns[m][i] = columns[m][i] - by * across[m - j - 1]
    return blocks[at] * lax.rsqrt(pivot)


def step_kernel(
    here_ref, there_ref, vec_ref, ict_ref, diag_ref, plan_ref,
    cols_ref, upd_ref, top_ref,
    padded, lower, remain,
):
    count, total = here_ref.shape[0], diag_ref.shape[0]
    k = vec_ref.shape[1]
    blk = vec_ref.shape[0] // total
    most = remain.shape[1] // blk
    cols_ref[...] = jnp.zeros(cols_ref.shape, F32)
    picked = (here_ref[:, pl.ds(0, k)] + there_ref[:, pl.ds(0, k)]).astype(BF16)
    padded[pl.ds(0, count), :] = jnp.zeros((count, k), BF16)
    padded[pl.ds(count, count), :] = picked
    ints = here_ref[:, pl.ds(k, LANES)] + there_ref[:, pl.ds(k, LANES)]
    schur = ints - dot_lanes(picked, padded[...])
    tile = (count, LANES)
    eye = jnp.where(iota(tile, 0) == iota(tile, 1), 1.0, 0.0)
    whole = jnp.where(iota(tile, 1) < count, eye, schur)
    panels = count // 8
    blocks = [whole[8 * i : 8 * i + 8] for i in range(panels)]
    chunk = 4
    places = [0, 1, 2]
    for at in range(panels):
        for first in [chunk * c for c, p in enumerate(places) if p == at]:
            starts = [pl.multiple_of(plan_ref[first + j] * blk, blk) for j in range(chunk)]
            part = jnp.concatenate([vec_ref[pl.ds(start, blk), :] for start in starts])
            prod = dot_lanes(picked, part)
            for j, start in enumerate(starts):
                remain[:, pl.ds((first + j) * blk, blk)] = (
                    ict_ref[:, pl.ds(start, blk)] - prod[:, j * blk : (j + 1) * blk]
                )
        lower[pl.ds(8 * at, 8), :] = eliminate(blocks, at)
    upd_ref[...] = diag_ref[...]
    high, low = halves(remain[...])
    lhigh, llow = halves(lower[:, pl.ds(0, count)])
    cols = dot(lhigh, high) + dot(lhigh, low) + dot(llow, high)
    top = jnp.zeros((1, blk), F32)
    for j in range(most):
        s = plan_ref[j]
        live = plan_ref[total + j] > 0
        mine = cols[:, j * blk : (j + 1) * blk]
        left = diag_ref[pl.ds(s, 1), :] - jnp.sum(mine * mine, axis=0, keepdims=True)
        left = jnp.where(iota((1, blk), 1) + s * blk == plan_ref[2 * total], 0.0, left)
        cols_ref[:, pl.ds(pl.multiple_of(s * blk, blk), blk)] = jnp.where(live, mine, 0.0)
        upd_ref[pl.ds(s, 1), :] = jnp.where(live, left, diag_ref[pl.ds(s, 1), :])
        top = jnp.maximum(top, jnp.where(live, left, 0.0))
    top_ref[...] = jnp.broadcast_to(top, top_ref.shape)


def step(here, there, vec, ict, diag, plan, copies):
    count, rows = ict.shape
    k = vec.shape[1]
    total = diag.shape[0]
    blk = rows // total
    most = min(LIVE_MOST, total)
    return pl.pallas_call(
        step_kernel,
        out_shape=(
            pltpu.VMEM((count, rows), F32),
            pltpu.VMEM((total, blk), F32),
            pltpu.VMEM((copies, blk), F32),
        ),
        in_specs=[VMEM, VMEM, VMEM, VMEM, VMEM, SMEM],
        out_specs=(VMEM, VMEM, VMEM),
        scratch_shapes=[
            pltpu.VMEM((2 * count, k), BF16),
            pltpu.VMEM((count, LANES), F32),
            pltpu.VMEM((count, most * blk), F32),
        ],
        compiler_params=pltpu.CompilerParams(vmem_limit_bytes=24 << 20),
        name="step",
    )(here, there, vec, ict, diag, plan)


def scale_kernel(tops_ref, upd_ref, held_ref, cols_ref, rel_ref, peak_ref, rel, top, sems):
    leaving = []
    for i, part in enumerate((pl.ds(0, 8), pl.ds(8, held_ref.shape[0] - 8))):
        leaving.append(
            pltpu.make_async_copy(held_ref.at[part, :], cols_ref.at[part, :], sems.at[i])
        )
        leaving[-1].start()
    peak = jnp.max(jnp.max(tops_ref[...], axis=0, keepdims=True), axis=1, keepdims=True)
    rel[...] = upd_ref[...] / peak
    top[...] = peak
    leaving.pop(0).wait()
    leaving.append(pltpu.make_async_copy(rel, rel_ref, sems.at[2]))
    leaving.append(pltpu.make_async_copy(top, peak_ref, sems.at[3]))
    leaving[-2].start()
    leaving[-1].start()
    for copy in leaving:
        copy.wait()


def scale(tops, upd, cols):
    return pl.pallas_call(
        scale_kernel,
        out_shape=(
            jax.ShapeDtypeStruct(cols.shape, F32),
            jax.ShapeDtypeStruct(upd.shape, F32),
            jax.ShapeDtypeStruct((1, 1), F32),
        ),
        in_specs=[VMEM, VMEM, VMEM],
        out_specs=(ANY, ANY, ANY),
        scratch_shapes=[
            pltpu.VMEM(upd.shape, F32),
            pltpu.VMEM((1, 1), F32),
            pltpu.SemaphoreType.DMA((4,)),
        ],
        compiler_params=pltpu.CompilerParams(vmem_limit_bytes=4 << 20),
        name="scale",
    )(tops, upd, cols)


def exchange(blocks, groups=None):
    return lax.all_to_all(
        blocks, "d", split_axis=0, concat_axis=0, axis_index_groups=groups, tiled=True
    )


def on_device(shape, vec, ints, diag, spb, live, pivots):
    count = pivots.shape[0]
    ict = ints.T
    at = np.arange(math.prod(shape)).reshape(shape)
    wide = [at[:, :, 0, x].ravel().tolist() for x in range(shape[3])]
    wide += [at[:, y, 1, :].ravel().tolist() for y in range(shape[1])]
    turns = []
    for k in range(1, shape[3]):
        to = np.stack([np.roll(at[:, :, 0], -k, 2), np.roll(at[:, :, 1], -k, 1)], 2)
        turns.append([(int(p), int(q)) for p, q in zip(at.ravel(), to.ravel())])
    mine, plan = pick(pivots[None, :], spb, live, vec, ict, len(wide[0]))
    sheet = exchange(mine, wide).reshape(len(wide[0]), -1)
    sheets = [sheet] + [lax.ppermute(sheet, "d", turn) for turn in turns]
    placed = place(sheets, count)
    pairs = [(int(p), int(q)) for p, q in zip(at.ravel(), at[:, :, ::-1].ravel())]
    other = lax.ppermute(placed, "d", pairs)
    cols, upd, top = step(
        placed, other, vec, ict, diag.reshape(live.shape[0], -1), plan, at.size
    )
    cols, rel, peak = scale(exchange(top), upd, cols)
    return (cols.T, rel.reshape(-1), peak.reshape(()))


def solution(mesh):
    shape = (8, 4, 2, mesh.shape["grp"])
    flat = Mesh(mesh.devices.reshape(-1), ("d",))
    d = P("d")
    return jax.shard_map(
        functools.partial(on_device, shape),
        mesh=flat,
        in_specs=(d, d, d, d, d, P()),
        out_specs=(d, d, P()),
        check_vma=False,
    )
```

```python
import functools
import math

import jax
import jax.numpy as jnp
import numpy as np
from jax import lax
from jax.experimental import pallas as pl
from jax.experimental.pallas import tpu as pltpu
from jax.sharding import Mesh
from jax.sharding import PartitionSpec as P

AXES = ("z", "y", "c", "x")
LANES = 128
LIVE_MOST = 12
VMEM = pl.BlockSpec(memory_space=pltpu.VMEM)
SMEM = pl.BlockSpec(memory_space=pltpu.SMEM)
ANY = pl.BlockSpec(memory_space=pltpu.HBM)
F32 = jnp.float32
BF16 = jnp.bfloat16


def iota(shape, dim):
    return lax.broadcasted_iota(jnp.int32, shape, dim)


def in_hbm(a):
    return pltpu.with_memory_space_constraint(a, pltpu.HBM)


def dot_lanes(a, b):
    return lax.dot_general(a, b, (((1,), (1,)), ((), ())), preferred_element_type=F32)


def dot(a, b):
    return lax.dot_general(a, b, (((1,), (0,)), ((), ())), preferred_element_type=F32)


def halves(a):
    hi = a.astype(BF16)
    return hi, (a - hi.astype(F32)).astype(BF16)


def pick_kernel(
    count, piv_ref, spb_ref, live_ref, vec_ref, ict_ref, out_ref, plan_ref, vbuf, ibuf, sems
):
    piv = piv_ref[...]
    group, offset = piv >> 7, piv & (LANES - 1)
    code = jnp.zeros(piv.shape, jnp.int32)
    for s in range(spb_ref.shape[0]):
        code = jnp.where(
            group == spb_ref[s], (s * LANES + offset) * count + iota(piv.shape, 1) + 1, code
        )
    best = jnp.max(code.astype(F32)).astype(jnp.int32)
    has = best > 0
    at = jnp.maximum(best - 1, 0)
    row, q = at // count, at % count
    vcopy = pltpu.make_async_copy(
        vec_ref.at[pl.ds(pl.multiple_of((row // 8) * 8, 8), 8), :], vbuf, sems.at[0]
    )
    icopy = pltpu.make_async_copy(
        ict_ref.at[:, pl.ds(pl.multiple_of((row // LANES) * LANES, LANES), LANES)],
        ibuf.at[pl.ds(count, count), :],
        sems.at[1],
    )
    vcopy.start()
    icopy.start()
    total = live_ref.shape[0]
    found = jnp.int32(0)
    for wanted in (1, 0):
        for s in range(total):
            plan_ref[found] = s
            plan_ref[total + found] = wanted
            found += (live_ref[s] > 0) == (wanted > 0)
    plan_ref[2 * total] = jnp.where(has, row, -1)
    ibuf[pl.ds(0, count), :] = jnp.zeros((count, LANES), F32)
    k = vbuf.shape[1]
    vcopy.wait()
    mine = (iota(vbuf.shape, 0) == row % 8) & has
    vrow = jnp.sum(jnp.where(mine, vbuf[...].astype(F32), 0.0), axis=0, keepdims=True)
    copies = out_ref.shape[0]
    for i in range(copies):
        out_ref[i, :, pl.ds(0, k)] = vrow
    icopy.wait()
    tile = (8, LANES)
    hot = jnp.where((iota(tile, 1) == row % LANES) & has, 1.0, 0.0).astype(BF16)
    rest, ints = ibuf[...], jnp.zeros(tile, F32)
    for _ in range(3):
        part = rest.astype(BF16)
        rest = rest - part.astype(F32)
        ints += dot_lanes(hot, part)
    index = jnp.where(has, q + 1, 0).astype(F32)
    tail = jnp.where(iota(tile, 1) == 0, index, ints)[0:1]
    for i in range(copies):
        out_ref[i, :, pl.ds(k, LANES)] = tail


def pick(pivots, spb, live, vec, ict, copies):
    count, k = pivots.shape[1], vec.shape[1]
    return pl.pallas_call(
        lambda *refs: pick_kernel(count, *refs),
        out_shape=(
            jax.ShapeDtypeStruct((copies, 1, k + LANES), F32),
            pltpu.SMEM((2 * live.shape[0] + 2,), jnp.int32),
        ),
        in_specs=[VMEM, SMEM, SMEM, ANY, ANY],
        out_specs=(VMEM, SMEM),
        scratch_shapes=[
            pltpu.VMEM((8, k), BF16),
            pltpu.VMEM((2 * count, LANES), F32),
            pltpu.SemaphoreType.DMA((2,)),
        ],
        compiler_params=pltpu.CompilerParams(vmem_limit_bytes=8 << 20),
        name="pick",
    )(in_hbm(pivots), in_hbm(spb), in_hbm(live), in_hbm(vec), in_hbm(ict))


def place_kernel(*refs):
    *sheets, out_ref = refs
    k = out_ref.shape[1] - LANES
    turn = (((0,), (0,)), ((), ()))
    total = jnp.zeros((out_ref.shape[0], LANES), F32)
    hots = []
    tails = []
    for ref in sheets:
        tail = ref[:, pl.ds(k, LANES)]
        hot = tail[:, 0:1].astype(jnp.int32) - 1 == iota((ref.shape[0], out_ref.shape[0]), 1)
        hots.append(jnp.where(hot, 1.0, 0.0).astype(BF16))
        tails.append(tail)
    hot, tail = jnp.concatenate(hots), jnp.concatenate(tails)
    body = jnp.concatenate([ref[:, pl.ds(0, k)].astype(BF16) for ref in sheets])
    out_ref[:, pl.ds(0, k)] = lax.dot_general(hot, body, turn, preferred_element_type=F32)
    for _ in range(3):
        part = tail.astype(BF16)
        tail = tail - part.astype(F32)
        total += lax.dot_general(hot, part, turn, preferred_element_type=F32)
    out_ref[:, pl.ds(k, LANES)] = total


def place(sheets, count):
    return pl.pallas_call(
        place_kernel,
        out_shape=jax.ShapeDtypeStruct((count, sheets[0].shape[1]), F32),
        in_specs=[VMEM] * len(sheets),
        out_specs=VMEM,
        compiler_params=pltpu.CompilerParams(vmem_limit_bytes=8 << 20),
        name="place",
    )(*sheets)


def eliminate(blocks, at):
    n = len(blocks)
    lead = 8 * n + 8 * at
    tile = blocks[0].shape
    columns = [
        {i: jnp.broadcast_to(blocks[i][:, lead + j : lead + j + 1], tile) for i in range(at, n)}
        for j in range(8)
    ]
    pivot = jnp.ones(tile, F32)
    for j in range(8):
        row = jnp.broadcast_to(blocks[at][j : j + 1], tile)
        d = jnp.broadcast_to(columns[j][at][j : j + 1], tile)
        inverse = 1.0 / d
        pivot = jnp.where(iota(tile, 0) == j, d, pivot)
        across = [jnp.broadcast_to(columns[m][at][j : j + 1], tile) for m in range(j + 1, 8)]
        for i in range(at, n):
            by = columns[j][i] * inverse
            if i == at:
                by = jnp.where(iota(tile, 0) > j, by, 0.0)
            blocks[i] = blocks[i] - by * row
            for m in range(j + 1, 8):
                columns[m][i] = columns[m][i] - by * across[m - j - 1]
    return blocks[at] * lax.rsqrt(pivot)


def step_kernel(
    here_ref, there_ref, vec_ref, ict_ref, diag_ref, plan_ref,
    cols_ref, upd_ref, top_ref,
    padded, lower, remain,
):
    count, total = here_ref.shape[0], diag_ref.shape[0]
    k = vec_ref.shape[1]
    blk = vec_ref.shape[0] // total
    most = remain.shape[1] // blk
    cols_ref[...] = jnp.zeros(cols_ref.shape, F32)
    picked = (here_ref[:, pl.ds(0, k)] + there_ref[:, pl.ds(0, k)]).astype(BF16)
    padded[pl.ds(0, count), :] = jnp.zeros((count, k), BF16)
    padded[pl.ds(count, count), :] = picked
    ints = here_ref[:, pl.ds(k, LANES)] + there_ref[:, pl.ds(k, LANES)]
    schur = ints - dot_lanes(picked, padded[...])
    tile = (count, LANES)
    eye = jnp.where(iota(tile, 0) == iota(tile, 1), 1.0, 0.0)
    whole = jnp.where(iota(tile, 1) < count, eye, schur)
    panels = count // 8
    blocks = [whole[8 * i : 8 * i + 8] for i in range(panels)]
    chunk = 4
    places = [0, 1, 2]
    for at in range(panels):
        for first in [chunk * c for c, p in enumerate(places) if p == at]:
            starts = [pl.multiple_of(plan_ref[first + j] * blk, blk) for j in range(chunk)]
            part = jnp.concatenate([vec_ref[pl.ds(start, blk), :] for start in starts])
            prod = dot_lanes(picked, part)
            for j, start in enumerate(starts):
                remain[:, pl.ds((first + j) * blk, blk)] = (
                    ict_ref[:, pl.ds(start, blk)] - prod[:, j * blk : (j + 1) * blk]
                )
        lower[pl.ds(8 * at, 8), :] = eliminate(blocks, at)
    upd_ref[...] = diag_ref[...]
    high, low = halves(remain[...])
    lhigh, llow = halves(lower[:, pl.ds(0, count)])
    cols = dot(lhigh, high) + dot(lhigh, low) + dot(llow, high)
    top = jnp.zeros((1, blk), F32)
    for j in range(most):
        s = plan_ref[j]
        live = plan_ref[total + j] > 0
        mine = cols[:, j * blk : (j + 1) * blk]
        left = diag_ref[pl.ds(s, 1), :] - jnp.sum(mine * mine, axis=0, keepdims=True)
        left = jnp.where(iota((1, blk), 1) + s * blk == plan_ref[2 * total], 0.0, left)
        cols_ref[:, pl.ds(pl.multiple_of(s * blk, blk), blk)] = jnp.where(live, mine, 0.0)
        upd_ref[pl.ds(s, 1), :] = jnp.where(live, left, diag_ref[pl.ds(s, 1), :])
        top = jnp.maximum(top, jnp.where(live, left, 0.0))
    top_ref[...] = jnp.broadcast_to(top, top_ref.shape)


def step(here, there, vec, ict, diag, plan, copies):
    count, rows = ict.shape
    k = vec.shape[1]
    total = diag.shape[0]
    blk = rows // total
    most = min(LIVE_MOST, total)
    return pl.pallas_call(
        step_kernel,
        out_shape=(
            pltpu.VMEM((count, rows), F32),
            pltpu.VMEM((total, blk), F32),
            pltpu.VMEM((copies, blk), F32),
        ),
        in_specs=[VMEM, VMEM, VMEM, VMEM, VMEM, SMEM],
        out_specs=(VMEM, VMEM, VMEM),
        scratch_shapes=[
            pltpu.VMEM((2 * count, k), BF16),
            pltpu.VMEM((count, LANES), F32),
            pltpu.VMEM((count, most * blk), F32),
        ],
        compiler_params=pltpu.CompilerParams(vmem_limit_bytes=24 << 20),
        name="step",
    )(here, there, vec, ict, diag, plan)


def scale_kernel(tops_ref, upd_ref, held_ref, cols_ref, rel_ref, peak_ref, rel, top, sems):
    leaving = []
    for i, part in enumerate((pl.ds(0, 8), pl.ds(8, held_ref.shape[0] - 8))):
        leaving.append(
            pltpu.make_async_copy(held_ref.at[part, :], cols_ref.at[part, :], sems.at[i])
        )
        leaving[-1].start()
    peak = jnp.max(jnp.max(tops_ref[...], axis=0, keepdims=True), axis=1, keepdims=True)
    rel[...] = upd_ref[...] / peak
    top[...] = peak
    leaving.pop(0).wait()
    leaving.append(pltpu.make_async_copy(rel, rel_ref, sems.at[2]))
    leaving.append(pltpu.make_async_copy(top, peak_ref, sems.at[3]))
    leaving[-2].start()
    leaving[-1].start()
    for copy in leaving:
        copy.wait()


def scale(tops, upd, cols):
    return pl.pallas_call(
        scale_kernel,
        out_shape=(
            jax.ShapeDtypeStruct(cols.shape, F32),
            jax.ShapeDtypeStruct(upd.shape, F32),
            jax.ShapeDtypeStruct((1, 1), F32),
        ),
        in_specs=[VMEM, VMEM, VMEM],
        out_specs=(ANY, ANY, ANY),
        scratch_shapes=[
            pltpu.VMEM(upd.shape, F32),
            pltpu.VMEM((1, 1), F32),
            pltpu.SemaphoreType.DMA((4,)),
        ],
        compiler_params=pltpu.CompilerParams(vmem_limit_bytes=4 << 20),
        name="scale",
    )(tops, upd, cols)


def exchange(blocks, groups=None):
    return lax.all_to_all(
        blocks, "d", split_axis=0, concat_axis=0, axis_index_groups=groups, tiled=True
    )


def on_device(shape, vec, ints, diag, spb, live, pivots):
    count = pivots.shape[0]
    ict = ints.T
    at = np.arange(math.prod(shape)).reshape(shape)
    wide = [at[:, :, 0, x].ravel().tolist() for x in range(shape[3])]
    wide += [at[:, y, 1, :].ravel().tolist() for y in range(shape[1])]
    turns = []
    for k in sorted(range(1, shape[3]), key=lambda k: min(k, shape[3] - k)):
        to = np.stack([np.roll(at[:, :, 0], -k, 2), np.roll(at[:, :, 1], -k, 1)], 2)
        turns.append([(int(p), int(q)) for p, q in zip(at.ravel(), to.ravel())])
    mine, plan = pick(pivots[None, :], spb, live, vec, ict, len(wide[0]))
    sheet = exchange(mine, wide).reshape(len(wide[0]), -1)
    sheets = [sheet] + [lax.ppermute(sheet, "d", turn) for turn in turns]
    placed = place(sheets, count)
    pairs = [(int(p), int(q)) for p, q in zip(at.ravel(), at[:, :, ::-1].ravel())]
    other = lax.ppermute(placed, "d", pairs)
    cols, upd, top = step(
        placed, other, vec, ict, diag.reshape(live.shape[0], -1), plan, at.size
    )
    cols, rel, peak = scale(exchange(top), upd, cols)
    return (cols.T, rel.reshape(-1), peak.reshape(()))


def solution(mesh):
    shape = (8, 4, 2, mesh.shape["grp"])
    flat = Mesh(mesh.devices.reshape(-1), ("d",))
    d = P("d")
    return jax.shard_map(
        functools.partial(on_device, shape),
        mesh=flat,
        in_specs=(d, d, d, d, d, P()),
        out_specs=(d, d, P()),
        check_vma=False,
    )
```
